512 devices in a mesh: dp: 64 (over z, y), mp: 8 (over x, core).
Axes of the slice: x: 4, y: 4, z: 16, core: 2. Of those that a mesh axis runs over, the one named last changes fastest.
Arguments:
- activations: bfloat16 [32768, 2048], P(('dp', 'mp')), may hold values from -400 to 400
- key_value_grads: bfloat16 [2, 32768, 1024], P(None, 'dp', 'mp'), may hold values from -320 to 320
- master_weights: float32 [2048, 2, 1024], P('dp', None, 'mp'), may hold values from -0.125 to 0.125
- first_moment: float32 [2048, 2, 1024], P('dp', None, 'mp'), may hold values from -0.005859375 to 0.005859375
- second_moment: float32 [2048, 2, 1024], P('dp', None, 'mp'), may hold values from 1e-08 to 1e-05
Outputs:
- master_out: float32 [2048, 2, 1024], P('dp', None, 'mp')
- first_out: float32 [2048, 2, 1024], P('dp', None, 'mp')
- second_out: float32 [2048, 2, 1024], P('dp', None, 'mp')
- weights_out: bfloat16 [2048, 2, 1024], P(None, None, 'mp')
The draws below stay inside these ranges and needn't reach their ends.
All inputs are finite; a program needn't handle non-finite values.
Results may differ from the reference program's by a relative error of at most 0.001.
Values may be sent and summed in bfloat16 or wider, within the bound.
A program may use at most 64 MiB of HBM per device.

```python
import math
import jax
import jax.numpy as jnp

D = 2048
STEP = 8
KV = 1024
TOKENS = 32768


def draw_activations(key, part):
    first_key, second_key = jax.random.split(jax.random.fold_in(key, 11), 2)
    normal_part = jnp.clip(jax.random.normal(first_key, (TOKENS, D), jnp.float32), -3.0, 3.0)
    columns = jnp.exp(jax.random.uniform(second_key, (D,), jnp.float32, 0.0, math.log(4.0)))
    columns = columns * 3.0 ** (jnp.arange(D, dtype=jnp.float32) / D)
    values = normal_part * columns
    return values.astype(jnp.bfloat16)


def draw_key_value_grads(key, part):
    first_key, second_key = jax.random.split(jax.random.fold_in(key, 23), 2)
    normal_part = jnp.clip(jax.random.normal(first_key, (2, TOKENS, KV), jnp.float32), -3.0, 3.0)
    columns = jnp.exp(jax.random.uniform(second_key, (2, 1, KV), jnp.float32, 0.0, math.log(10.0)))
    values = normal_part * columns
    return values.astype(jnp.bfloat16)


def block_levels(key, shape, cuts, smallest, top_value):
    level = 1.0
    for axis_at, shards_of in cuts:
        heights = jax.random.uniform(jax.random.fold_in(jax.random.fold_in(key, 6), axis_at), (shards_of,), jnp.float32, smallest / len(cuts), top_value / len(cuts))
        level = level * jnp.repeat(jnp.exp(heights), shape[axis_at] // shards_of).reshape((-1,) + (1,) * (len(shape) - 1 - axis_at))
    return level


def scatter_about(own_key, shape, spread, bound, cuts=(), held_as=jnp.bfloat16):
    loudness = block_levels(own_key, shape, cuts, -0.22, 0.18) if cuts else 1.0
    drawn = jax.random.normal(own_key, shape, jnp.float32) * spread * loudness
    return jnp.minimum(jnp.maximum(drawn, -bound), bound).astype(held_as)


def setup_inputs(seed: int = 0) -> dict:
    splits = jax.random.split(jax.random.key(seed), 6)
    activations = draw_activations(jax.random.fold_in(splits[5], 71), 0)
    key_value_grads = draw_key_value_grads(jax.random.fold_in(splits[5], 71), 0)
    master_weights = scatter_about(splits[2], (D, 2, KV), D ** -0.5, 0.125, ((0, 64), (2, 8)), jnp.float32)
    first_moment = scatter_about(splits[3], (D, 2, KV), 0.001, 0.005859375, ((0, 64), (2, 8)), jnp.float32)
    second_moment = jnp.clip(jnp.exp(math.log(9.999999747378752e-06) - 6.9077553 * jax.random.uniform(splits[4], (D, 2, KV), jnp.float32) ** block_levels(splits[4], (D, 2, KV), ((0, 64), (2, 8)), -0.2, 0.2)), 9.99999993922529e-09, 9.999999747378752e-06)
    return dict(activations=activations, key_value_grads=key_value_grads, master_weights=master_weights, first_moment=first_moment, second_moment=second_moment)


beta_first = 0.9
beta_second = 0.95
adam_epsilon = 1e-08
learning_rate = 0.001
weight_decay = 0.1
clip_scale = 0.001

def reference(activations, key_value_grads, master_weights, first_moment, second_moment):
    pieces = [jnp.dot(activations.T, key_value_grads[which], preferred_element_type=jnp.float32) for which in range(2)]
    gradient = jnp.stack(pieces, axis=1) / TOKENS
    total_squares = jnp.sum(gradient * gradient)
    grad_norm = jnp.sqrt(total_squares)
    limit = clip_scale * math.sqrt(2.0 * D * KV)
    clip_factor = jnp.minimum(jnp.float32(1.0), limit / (grad_norm + 1e-06))
    clipped = clip_factor * gradient
    first_out = beta_first * first_moment + (1.0 - beta_first) * clipped
    second_out = beta_second * second_moment + (1.0 - beta_second) * clipped * clipped
    first_hat = first_out / (1.0 - beta_first ** STEP)
    second_hat = second_out / (1.0 - beta_second ** STEP)
    master_out = master_weights - learning_rate * (first_hat / (jnp.sqrt(second_hat) + adam_epsilon) + weight_decay * master_weights)
    weights_out = master_out.astype(jnp.bfloat16)
    return (master_out, first_out, second_out, weights_out)
```

```python
import math

import jax
import jax.numpy as jnp
from jax import lax
from jax.experimental import pallas as pl
from jax.experimental.pallas import tpu as pltpu
from jax.sharding import Mesh
from jax.sharding import PartitionSpec as P

D = 2048
STEP = 8
KV = 1024
NZ, NY, NX, NC = 16, 4, 4, 2
STEPS = 8
DP = ("z", "y")
MP = ("x", "c")
DP_MP = ("z", "y", "x", "c")
MESH_ID = pl.DeviceIdType.MESH

beta_first = 0.9
beta_second = 0.95
adam_epsilon = 1e-08
learning_rate = 0.001
weight_decay = 0.1
clip_scale = 0.001

GROUP = [(dx, dc) for dc in range(NC) for dx in range(NX) if (dx, dc) != (0, 0)]


def step_kernel(
    acts_hbm, grads_hbm, master_hbm, first_hbm, second_hbm,
    master_out, first_out, second_out, weights_out,
    acts, slabs, cols, part, ysend, yrecv, zsend, zrecv, half, peer_half,
    nsend, nrecv_g, nrecv_y, nrecv_z,
    master, first, second, wide, rows_out, wbuf,
    load_sem, own_sem, grad_sem, state_sem, swap_send, swap_recv,
    xsend_sem, xrecv_sem, ysend_sem, yrecv_sem, zsend_sem, zrecv_sem,
    half_send, half_recv, nsend_sem, nrecv_sem, gsend_sem, gz_sem, gy_sem, out_sem,
):
    z, y, x, c = (lax.axis_index(a) for a in DP_MP)
    dp = z * NY + y
    mp = x * NC + c

    def at_z(k):
        return (lax.rem(z + k, NZ), y, x, c)

    def at_y(k):
        return (z, lax.rem(y + k, NY), x, c)

    def at_group(dx, dc):
        return (z, y, lax.rem(x + dx, NX), lax.rem(c + dc, NC))

    def block_of(i, core):
        return lax.rem(z + jnp.where(core == 0, 8 + i, 7 - i), NZ)

    def send(src, dst, send_sem, recv_sem, device):
        copy = pltpu.make_async_remote_copy(
            src_ref=src, dst_ref=dst, send_sem=send_sem, recv_sem=recv_sem,
            device_id=device, device_id_type=MESH_ID,
        )
        copy.start()

    def wait_bytes(ref, sem):
        pltpu.make_async_copy(ref, ref, sem).wait()

    barrier = pltpu.get_barrier_semaphore()
    for k in range(1, NZ):
        pl.semaphore_signal(barrier, inc=1, device_id=at_z(k), device_id_type=MESH_ID)
    for k in range(1, NY):
        pl.semaphore_signal(barrier, inc=1, device_id=at_y(k), device_id_type=MESH_ID)
    for dx, dc in GROUP:
        pl.semaphore_signal(barrier, inc=1, device_id=at_group(dx, dc), device_id_type=MESH_ID)

    own_rows = pl.ds(pl.multiple_of(mp * 64, 64), 64)
    own_cols = pl.ds(pl.multiple_of(c * 256, 256), 256)
    for b in range(NZ):
        pltpu.make_async_copy(acts_hbm.at[:, pl.ds(b * 128, 128)], acts.at[b], load_sem).start()
    for which in range(2):
        lanes = pl.ds(pl.multiple_of(c * 256 + which * 128, 128), 128)
        pltpu.make_async_copy(grads_hbm.at[which], cols.at[:, lanes], grad_sem).start()
    for i in range(STEPS):
        lanes = pl.ds(pl.multiple_of(block_of(i, c) * 128, 128), 128)
        pltpu.make_async_copy(acts_hbm.at[:, lanes], slabs.at[i, own_rows], own_sem).start()
    pltpu.make_async_copy(master_hbm, master, state_sem.at[0]).start()
    pltpu.make_async_copy(first_hbm, first, state_sem.at[1]).start()
    pltpu.make_async_copy(second_hbm, second, state_sem.at[2]).start()

    wait_bytes(acts, load_sem)
    wait_bytes(cols.at[:, pl.ds(0, 256)], grad_sem)
    pl.semaphore_wait(barrier, (NZ - 1) + (NY - 1) + len(GROUP))

    send(cols.at[:, own_cols], cols.at[:, own_cols], swap_send, swap_recv, at_group(0, 1))

    def gather_step(i, carry):
        for core in range(NC):
            slab = acts.at[block_of(i, core)]
            for dx in range(1, NX):
                send(slab, slabs.at[i, own_rows], xsend_sem, xrecv_sem.at[i],
                     (z, y, lax.rem(x + dx, NX), core))
        slab = acts.at[block_of(i, 1 - c)]
        send(slab, slabs.at[i, own_rows], xsend_sem, xrecv_sem.at[i], (z, y, x, 1 - c))
        return carry

    lax.fori_loop(0, STEPS, gather_step, 0)

    wait_bytes(slabs.at[:, pl.ds(0, 64)], own_sem)
    wait_bytes(cols.at[:, pl.ds(0, 256)], swap_recv)

    def multiply(i):
        wait_bytes(slabs.at[i, pl.ds(0, 448)], xrecv_sem.at[i])
        part[i % 2] = lax.dot_general(
            slabs[i], cols[...], (((0,), (0,)), ((), ())), preferred_element_type=jnp.float32
        )
        for k in range(1, NY):
            rows = pl.ds(pl.multiple_of(lax.rem(y + k, NY) * 32, 32), 32)
            piece = part[i % 2, rows, :].astype(jnp.bfloat16)
            for core in range(NC):
                for which in range(2):
                    at = core * 256 + which * 128
                    ysend[i, k - 1, core, which * 32 : which * 32 + 32, :] = piece[:, at : at + 128]
        for k in range(1, NY):
            send(ysend.at[i, k - 1], yrecv.at[i, k - 1], ysend_sem, yrecv_sem.at[i], at_y(k))

    def pass_on(i):
        wait_bytes(yrecv.at[i], yrecv_sem.at[i])
        rows = pl.ds(pl.multiple_of(y * 32, 32), 32)
        for core in range(NC):
            for which in range(2):
                at = core * 256 + which * 128
                total = part[i % 2, rows, at : at + 128]
                for k in range(NY - 1):
                    total += yrecv[i, k, core, which * 32 : which * 32 + 32, :].astype(jnp.float32)
                zsend[i, core, which * 32 : which * 32 + 32, :] = total.astype(jnp.bfloat16)
        k = jnp.where(c == 0, 8 + i, 7 - i)

        @pl.when(k != 0)
        def _():
            send(zsend.at[i], zrecv.at[i], zsend_sem, zrecv_sem.at[i], at_z(k))

    multiply(0)

    def reduce_step(i, carry):
        multiply(i)
        pass_on(i - 1)
        return carry

    lax.fori_loop(1, STEPS, reduce_step, 0)
    pass_on(STEPS - 1)

    for core in range(NC):
        half[core] = jnp.zeros((64, 128), jnp.float32)

    def collect(i):
        wait_bytes(zrecv.at[i], zrecv_sem.at[i])
        for core in range(NC):
            half[core] += zrecv[i, core].astype(jnp.float32)

    for i in range(STEPS - 1):
        collect(i)

    @pl.when(c == 0)
    def _():
        collect(STEPS - 1)

    @pl.when(c == 1)
    def _():
        for core in range(NC):
            half[core] += zsend[STEPS - 1, core].astype(jnp.float32)

    send(half.at[1 - c], peer_half, half_send, half_recv, at_group(0, 1))
    wait_bytes(peer_half, half_recv)

    tokens = 64 * NX * NC * NZ * NY
    gradient = (half[c] + peer_half[...]) * (1.0 / tokens)

    squares = jnp.sum(gradient * gradient, axis=0, keepdims=True)
    nsend[0] = squares
    for n, (dx, dc) in enumerate(GROUP):
        send(nsend.at[0], nrecv_g.at[n], nsend_sem.at[0], nrecv_sem.at[0], at_group(dx, dc))
    wait_bytes(nrecv_g, nrecv_sem.at[0])
    for n in range(len(GROUP)):
        squares += nrecv_g[n]
    nsend[1] = squares
    for k in range(1, NY):
        send(nsend.at[1], nrecv_y.at[k - 1], nsend_sem.at[1], nrecv_sem.at[1], at_y(k))
    wait_bytes(nrecv_y, nrecv_sem.at[1])
    for k in range(NY - 1):
        squares += nrecv_y[k]
    nsend[2] = squares
    for k in (8, 7, 9, 6, 10, 5, 11, 4, 12, 3, 13, 2, 14, 1, 15):
        send(nsend.at[2], nrecv_z.at[k - 1], nsend_sem.at[2], nrecv_sem.at[2], at_z(k))
    for n in range(3):
        wait_bytes((master, first, second)[n], state_sem.at[n])
    wait_bytes(nrecv_z, nrecv_sem.at[2])
    for k in range(NZ - 1):
        squares += nrecv_z[k]

    grad_norm = jnp.sqrt(jnp.sum(squares, axis=1, keepdims=True))
    limit = clip_scale * math.sqrt(2.0 * D * KV)
    clip_factor = jnp.minimum(jnp.float32(1.0), limit / (grad_norm + 1e-06))
    clipped_all = clip_factor * gradient
    for which in range(2):
        pick = pl.ds(which, 32, stride=2)
        clipped = clipped_all[which * 32 : which * 32 + 32]
        weights = master[pick, :]
        m = beta_first * first[pick, :] + (1.0 - beta_first) * clipped
        v = beta_second * second[pick, :] + (1.0 - beta_second) * clipped * clipped
        first_hat = m / (1.0 - beta_first**STEP)
        second_hat = v / (1.0 - beta_second**STEP)
        new = weights - learning_rate * (
            first_hat / (jnp.sqrt(second_hat) + adam_epsilon) + weight_decay * weights
        )
        rows_out[0, pick, :] = new
        rows_out[1, pick, :] = m
        rows_out[2, pick, :] = v
    wbuf[dp] = rows_out[0].astype(jnp.bfloat16)

    own = wbuf.at[dp]
    for n, k in enumerate((8, 7, 9, 6, 10, 5, 11, 4, 12, 3, 13, 2, 14, 1, 15)):
        send(own, own, gsend_sem, gz_sem.at[n], at_z(k))
    for k in range(1, NY):
        send(own, own, gsend_sem, gy_sem, at_y(k))
    for n, out in enumerate((master_out, first_out, second_out)):
        pltpu.make_async_copy(rows_out.at[n], out, out_sem.at[n]).start()
    for n, k in enumerate((8, 7, 9, 6, 10, 5, 11, 4, 12, 3, 13, 2, 14, 1, 15)):
        got = wbuf.at[lax.rem(z + NZ - k, NZ) * NY + y]
        wait_bytes(got, gz_sem.at[n])
        for k_y in range(1, NY):
            send(got, got, gsend_sem, gy_sem, at_y(k_y))
    wait_bytes(wbuf.at[pl.ds(0, 48)], gy_sem)
    pltpu.make_async_copy(wbuf, weights_out, out_sem.at[3]).start()

    wait_bytes(cols.at[:, pl.ds(0, 256)], swap_send)
    wait_bytes(slabs.at[pl.ds(0, 7)], xsend_sem)
    wait_bytes(yrecv, ysend_sem)
    wait_bytes(zsend.at[pl.ds(0, 7)], zsend_sem)

    @pl.when(c == 0)
    def _():
        wait_bytes(zsend.at[7], zsend_sem)

    wait_bytes(peer_half, half_send)
    wait_bytes(nrecv_g, nsend_sem.at[0])
    wait_bytes(nrecv_y, nsend_sem.at[1])
    wait_bytes(nrecv_z, nsend_sem.at[2])
    wait_bytes(wbuf.at[pl.ds(0, 63)], gsend_sem)
    for n in range(3):
        pltpu.make_async_copy(rows_out.at[n], (master_out, first_out, second_out)[n], out_sem.at[n]).wait()
    pltpu.make_async_copy(wbuf, weights_out, out_sem.at[3]).wait()


def on_device(activations, key_value_grads, master_weights, first_moment, second_moment):
    f32, bf16 = jnp.float32, jnp.bfloat16
    any_space = pl.BlockSpec(memory_space=pl.ANY)
    dma = pltpu.SemaphoreType.DMA
    vmem = pltpu.VMEM
    flat = [a.reshape(64, 128) for a in (master_weights, first_moment, second_moment)]
    outs = pl.pallas_call(
        step_kernel,
        out_shape=[jax.ShapeDtypeStruct((64, 128), f32)] * 3 + [jax.ShapeDtypeStruct((64, 64, 128), bf16)],
        in_specs=[any_space] * 5,
        out_specs=[any_space] * 4,
        scratch_shapes=[
            vmem((NZ, 64, 128), bf16),
            vmem((STEPS, 512, 128), bf16),
            vmem((512, 512), bf16),
            vmem((2, 128, 512), f32),
            vmem((STEPS, NY - 1, NC, 64, 128), bf16),
            vmem((STEPS, NY - 1, NC, 64, 128), bf16),
            vmem((STEPS, NC, 64, 128), bf16),
            vmem((STEPS, NC, 64, 128), bf16),
            vmem((NC, 64, 128), f32),
            vmem((64, 128), f32),
            vmem((3, 1, 128), f32),
            vmem((len(GROUP), 1, 128), f32),
            vmem((NY - 1, 1, 128), f32),
            vmem((NZ - 1, 1, 128), f32),
            vmem((64, 128), f32),
            vmem((64, 128), f32),
            vmem((64, 128), f32),
            vmem((64, 128), f32),
            vmem((3, 64, 128), f32),
            vmem((64, 64, 128), bf16),
            dma, dma, dma, dma((3,)), dma, dma,
            dma, dma((STEPS,)), dma, dma((STEPS,)), dma, dma((STEPS,)),
            dma, dma, dma((3,)), dma((3,)), dma, dma((NZ - 1,)), dma, dma((4,)),
        ],
        compiler_params=pltpu.CompilerParams(collective_id=0, has_side_effects=True),
        name="adam_step",
    )(activations, key_value_grads, *flat)
    return tuple(o.reshape(32, 2, 128) for o in outs[:3]) + (outs[3].reshape(D, 2, 128),)


def solution(mesh):
    split = Mesh(mesh.devices.reshape(NZ, NY, NX, NC), DP_MP)
    return jax.shard_map(
        on_device,
        mesh=split,
        in_specs=(
            P(DP_MP, None),
            P(None, DP, MP),
            P(DP, None, MP),
            P(DP, None, MP),
            P(DP, None, MP),
        ),
        out_specs=(P(DP, None, MP), P(DP, None, MP), P(DP, None, MP), P(None, None, MP)),
        check_vma=False,
    )
```

```python
import math

import jax
import jax.numpy as jnp
from jax import lax
from jax.experimental import pallas as pl
from jax.experimental.pallas import tpu as pltpu
from jax.sharding import Mesh
from jax.sharding import PartitionSpec as P

D = 2048
STEP = 8
KV = 1024
NZ, NY, NX, NC = 16, 4, 4, 2
STEPS = 8
AHEAD = 3
LAG = 2
PARTS = LAG + 1
DP = ("z", "y")
MP = ("x", "c")
DP_MP = ("z", "y", "x", "c")
MESH_ID = pl.DeviceIdType.MESH

beta_first = 0.9
beta_second = 0.95
adam_epsilon = 1e-08
learning_rate = 0.001
weight_decay = 0.1
clip_scale = 0.001

PLANE = [(dy, dx, dc) for dy in range(NY) for dx in range(NX) for dc in range(NC) if (dy, dx, dc) != (0, 0, 0)]
Z_ORDER = (8, 7, 9, 6, 10, 5, 11, 4, 12, 3, 13, 2, 14, 1, 15)
SPREAD = (4, -4, 1, -1, 2, -2, 3, -3)
ARRIVAL = (1, -1, 4, -4, 2, -2, 3, -3, 5, -5, 6, -6, 7, -7, 8)


def step_kernel(
    acts_hbm, grads_hbm, master_hbm, first_hbm, second_hbm,
    master_out, first_out, second_out, wbuf,
    acts, slabs, cols, part, ysend, yrecv, zsend, zrecv,
    nsend, nrecv_p, nrecv_z,
    master, first, second,
    load_sem, own_sem, grad_sem, state_sem, swap_send, swap_recv,
    xsend_sem, xrecv_sem, ysend_sem, yrecv_sem, zsend_sem, zrecv_sem,
    nsend_sem, nrecv_sem, gsend_sem, gz_sem, gy_sem,
):
    z, y, x, c = (lax.axis_index(a) for a in DP_MP)
    dp = z * NY + y
    mp = x * NC + c

    def at_z(k):
        return (lax.rem(z + k, NZ), y, x, c)

    def at_y(k):
        return (z, lax.rem(y + k, NY), x, c)

    def in_plane(dy, dx, dc):
        return (z, lax.rem(y + dy, NY), lax.rem(x + dx, NX), lax.rem(c + dc, NC))

    def block_of(i, core):
        return lax.rem(z + jnp.where(core == 0, 8 + i, 7 - i), NZ)

    def send(src, dst, send_sem, recv_sem, device):
        copy = pltpu.make_async_remote_copy(
            src_ref=src, dst_ref=dst, send_sem=send_sem, recv_sem=recv_sem,
            device_id=device, device_id_type=MESH_ID,
        )
        copy.start()

    def wait_bytes(ref, sem):
        pltpu.make_async_copy(ref, ref, sem).wait()

    barrier = pltpu.get_barrier_semaphore()
    for k in Z_ORDER:
        for core in range(NC):
            pl.semaphore_signal(barrier, inc=1, device_id=(lax.rem(z + k, NZ), y, x, core), device_id_type=MESH_ID)
    for d in PLANE:
        pl.semaphore_signal(barrier, inc=1, device_id=in_plane(*d), device_id_type=MESH_ID)

    own_rows = pl.ds(pl.multiple_of(mp * 64, 64), 64)
    own_cols = pl.ds(pl.multiple_of(c * 256, 256), 256)
    for b in range(NZ):
        pltpu.make_async_copy(acts_hbm.at[:, pl.ds(b * 128, 128)], acts.at[b], load_sem).start()
    for which in range(2):
        lanes = pl.ds(pl.multiple_of(c * 256 + which * 128, 128), 128)
        pltpu.make_async_copy(grads_hbm.at[which], cols.at[:, lanes], grad_sem).start()
    for i in range(STEPS):
        lanes = pl.ds(pl.multiple_of(block_of(i, c) * 128, 128), 128)
        pltpu.make_async_copy(acts_hbm.at[:, lanes], slabs.at[i, own_rows], own_sem).start()
    pltpu.make_async_copy(master_hbm, master, state_sem.at[0]).start()
    pltpu.make_async_copy(first_hbm, first, state_sem.at[1]).start()
    pltpu.make_async_copy(second_hbm, second, state_sem.at[2]).start()

    wait_bytes(acts, load_sem)
    wait_bytes(cols.at[:, pl.ds(0, 256)], grad_sem)
    pl.semaphore_wait(barrier, NC * (NZ - 1) + len(PLANE))

    send(cols.at[:, own_cols], cols.at[:, own_cols], swap_send, swap_recv, in_plane(0, 0, 1))

    def gather_step(i):
        for core in range(NC):
            slab = acts.at[block_of(i, core)]
            for dx in range(1, NX):
                send(slab, slabs.at[i, own_rows], xsend_sem, xrecv_sem.at[i],
                     (z, y, lax.rem(x + dx, NX), core))
        slab = acts.at[block_of(i, 1 - c)]
        send(slab, slabs.at[i, own_rows], xsend_sem, xrecv_sem.at[i], (z, y, x, 1 - c))

    for i in range(AHEAD):
        gather_step(i)

    wait_bytes(slabs.at[:, pl.ds(0, 64)], own_sem)
    wait_bytes(cols.at[:, pl.ds(0, 256)], swap_recv)

    def multiply(i):
        wait_bytes(slabs.at[i, pl.ds(0, 448)], xrecv_sem.at[i])

        @pl.when(i + AHEAD < STEPS)
        def _():
            gather_step(i + AHEAD)

        part[i % PARTS] = lax.dot_general(
            slabs[i], cols[...], (((0,), (0,)), ((), ())), preferred_element_type=jnp.float32
        )
        for k in range(1, NY):
            rows = pl.ds(pl.multiple_of(lax.rem(y + k, NY) * 32, 32), 32)
            piece = part[i % PARTS, rows, :].astype(jnp.bfloat16)
            for core in range(NC):
                for which in range(2):
                    at = core * 256 + which * 128
                    ysend[i, k - 1, core, which * 32 : which * 32 + 32, :] = piece[:, at : at + 128]
        for k in range(1, NY):
            send(ysend.at[i, k - 1], yrecv.at[i, k - 1], ysend_sem, yrecv_sem.at[i], at_y(k))

    def pass_on(i):
        wait_bytes(yrecv.at[i], yrecv_sem.at[i])
        rows = pl.ds(pl.multiple_of(y * 32, 32), 32)
        for core in range(NC):
            for which in range(2):
                at = core * 256 + which * 128
                total = part[i % PARTS, rows, at : at + 128]
                for k in range(NY - 1):
                    total += yrecv[i, k, core, which * 32 : which * 32 + 32, :].astype(jnp.float32)
                zsend[i, core, which * 32 : which * 32 + 32, :] = total.astype(jnp.bfloat16)
        k = jnp.where(c == 0, 8 + i, 7 - i)

        slot = 2 * i + c
        send(zsend.at[i, 0], zrecv.at[slot], zsend_sem, zrecv_sem.at[slot], (lax.rem(z + k, NZ), y, x, 0))

        @pl.when(k != 0)
        def _():
            send(zsend.at[i, 1], zrecv.at[slot], zsend_sem, zrecv_sem.at[slot], (lax.rem(z + k, NZ), y, x, 1))

    for i in range(LAG):
        multiply(i)

    def reduce_step(i, carry):
        multiply(i)
        pass_on(i - LAG)
        return carry

    lax.fori_loop(LAG, STEPS, reduce_step, 0)
    for i in range(STEPS - LAG, STEPS):
        pass_on(i)

    @pl.when(c == 1)
    def _():
        zrecv[NZ - 1] = zsend[STEPS - 1, 1]

    @pl.when(c == 0)
    def _():
        wait_bytes(zrecv.at[NZ - 1], zrecv_sem.at[NZ - 1])

    total = jnp.zeros((64, 128), jnp.float32)
    for slot in range(NZ - 1):
        wait_bytes(zrecv.at[slot], zrecv_sem.at[slot])
        total += zrecv[slot].astype(jnp.float32)
    total += zrecv[NZ - 1].astype(jnp.float32)

    tokens = 64 * NX * NC * NZ * NY
    gradient = total * (1.0 / tokens)

    squares = jnp.sum(gradient * gradient, axis=0, keepdims=True)
    nsend[0] = squares
    for n, d in enumerate(PLANE):
        send(nsend.at[0], nrecv_p.at[n], nsend_sem.at[0], nrecv_sem.at[0], in_plane(*d))
    wait_bytes(nrecv_p, nrecv_sem.at[0])
    squares += jnp.sum(nrecv_p[...], axis=0)
    nsend[1] = squares
    for k in Z_ORDER:
        send(nsend.at[1], nrecv_z.at[k - 1], nsend_sem.at[1], nrecv_sem.at[1], at_z(k))
    for n in range(3):
        wait_bytes((master, first, second)[n], state_sem.at[n])
    wait_bytes(nrecv_z, nrecv_sem.at[1])
    squares += jnp.sum(nrecv_z[...], axis=0)

    grad_norm = jnp.sqrt(jnp.sum(squares, axis=1, keepdims=True))
    limit = clip_scale * math.sqrt(2.0 * D * KV)
    clip_factor = jnp.minimum(jnp.float32(1.0), limit / (grad_norm + 1e-06))
    clipped_all = clip_factor * gradient
    for which in range(2):
        pick = pl.ds(which, 32, stride=2)
        clipped = clipped_all[which * 32 : which * 32 + 32]
        weights = master[pick, :]
        m = beta_first * first[pick, :] + (1.0 - beta_first) * clipped
        v = beta_second * second[pick, :] + (1.0 - beta_second) * clipped * clipped
        first_hat = m / (1.0 - beta_first**STEP)
        second_hat = v / (1.0 - beta_second**STEP)
        new = weights - learning_rate * (
            first_hat / (jnp.sqrt(second_hat) + adam_epsilon) + weight_decay * weights
        )
        master_out[pick, :] = new
        first_out[pick, :] = m
        second_out[pick, :] = v
    wbuf[dp] = master_out[...].astype(jnp.bfloat16)

    own = wbuf.at[dp]
    side = jnp.where(c == 0, 1, NZ - 1)

    def along(k):
        return lax.rem(z + side * (k + NZ), NZ)

    def pass_along(block, k, by):
        send(block, block, gsend_sem, gz_sem.at[ARRIVAL.index(k)], (along(by), y, x, c))

    def pass_across(block):
        for k in range(1, NY):
            send(block, block, gsend_sem, gy_sem, at_y(k))

    for k in SPREAD:
        pass_along(own, k, k)
    pass_across(own)
    for n, k in enumerate(ARRIVAL):
        got = wbuf.at[along(-k) * NY + y]
        wait_bytes(got, gz_sem.at[n])
        if k == 4:
            for by in (4, 3, 2, 1):
                pass_along(got, 4 + by, by)
        if k == -4:
            for by in (3, 2, 1):
                pass_along(got, -4 - by, -by)
        pass_across(got)
    wait_bytes(wbuf.at[pl.ds(0, 48)], gy_sem)

    wait_bytes(cols.at[:, pl.ds(0, 256)], swap_send)
    wait_bytes(slabs.at[pl.ds(0, 7)], xsend_sem)
    wait_bytes(yrecv, ysend_sem)
    wait_bytes(zrecv.at[pl.ds(0, NZ - 1)], zsend_sem)

    @pl.when(c == 0)
    def _():
        wait_bytes(zrecv.at[NZ - 1], zsend_sem)

    wait_bytes(nrecv_p, nsend_sem.at[0])
    wait_bytes(nrecv_z, nsend_sem.at[1])
    wait_bytes(wbuf.at[pl.ds(0, 63)], gsend_sem)


def write_kernel(*refs):
    ins, outs, sem = refs[:4], refs[4:8], refs[8]
    copies = [pltpu.make_async_copy(i, o, sem.at[n]) for n, (i, o) in enumerate(zip(ins, outs))]
    for copy in copies:
        copy.start()
    for copy in copies:
        copy.wait()


def on_device(activations, key_value_grads, master_weights, first_moment, second_moment):
    f32, bf16 = jnp.float32, jnp.bfloat16
    any_space = pl.BlockSpec(memory_space=pl.ANY)
    dma = pltpu.SemaphoreType.DMA
    vmem = pltpu.VMEM
    flat = [a.reshape(64, 128) for a in (master_weights, first_moment, second_moment)]
    in_vmem = pl.BlockSpec(memory_space=pltpu.VMEM)
    results = pl.pallas_call(
        step_kernel,
        out_shape=[vmem((64, 128), f32)] * 3 + [vmem((64, 64, 128), bf16)],
        in_specs=[any_space] * 5,
        out_specs=[in_vmem] * 4,
        scratch_shapes=[
            vmem((NZ, 64, 128), bf16),
            vmem((STEPS, 512, 128), bf16),
            vmem((512, 512), bf16),
            vmem((PARTS, 128, 512), f32),
            vmem((STEPS, NY - 1, NC, 64, 128), bf16),
            vmem((STEPS, NY - 1, NC, 64, 128), bf16),
            vmem((STEPS, NC, 64, 128), bf16),
            vmem((NZ, 64, 128), bf16),
            vmem((2, 1, 128), f32),
            vmem((len(PLANE), 1, 128), f32),
            vmem((NZ - 1, 1, 128), f32),
            vmem((64, 128), f32),
            vmem((64, 128), f32),
            vmem((64, 128), f32),
            dma, dma, dma, dma((3,)), dma, dma,
            dma, dma((STEPS,)), dma, dma((STEPS,)), dma, dma((NZ,)),
            dma((2,)), dma((2,)), dma, dma((NZ - 1,)), dma,
        ],
        compiler_params=pltpu.CompilerParams(collective_id=0, has_side_effects=True),
        name="adam_step",
    )(activations, key_value_grads, *flat)
    results = [pltpu.with_memory_space_constraint(r, pltpu.VMEM) for r in results]
    outs = pl.pallas_call(
        write_kernel,
        out_shape=[jax.ShapeDtypeStruct((64, 128), f32)] * 3 + [jax.ShapeDtypeStruct((64, 64, 128), bf16)],
        in_specs=[any_space] * 4,
        out_specs=[any_space] * 4,
        scratch_shapes=[dma((4,))],
        name="write_out",
    )(*results)
    return tuple(o.reshape(32, 2, 128) for o in outs[:3]) + (outs[3].reshape(D, 2, 128),)


def solution(mesh):
    split = Mesh(mesh.devices.reshape(NZ, NY, NX, NC), DP_MP)
    return jax.shard_map(
        on_device,
        mesh=split,
        in_specs=(
            P(DP_MP, None),
            P(None, DP, MP),
            P(DP, None, MP),
            P(DP, None, MP),
            P(DP, None, MP),
        ),
        out_specs=(P(DP, None, MP), P(DP, None, MP), P(DP, None, MP), P(None, None, MP)),
        check_vma=False,
    )
```

```python
import math

import jax
import jax.numpy as jnp
from jax import lax
from jax.experimental import pallas as pl
from jax.experimental.pallas import tpu as pltpu
from jax.sharding import Mesh
from jax.sharding import PartitionSpec as P

D = 2048
STEP = 8
KV = 1024
NZ, NY, NX, NC = 16, 4, 4, 2
STEPS = 8
AHEAD = 3
LAG = 2
PARTS = LAG + 1
DP = ("z", "y")
MP = ("x", "c")
DP_MP = ("z", "y", "x", "c")
MESH_ID = pl.DeviceIdType.MESH

beta_first = 0.9
beta_second = 0.95
adam_epsilon = 1e-08
learning_rate = 0.001
weight_decay = 0.1
clip_scale = 0.001

PLANE = NY * NX * NC
Z_ORDER = (8, 7, 9, 6, 10, 5, 11, 4, 12, 3, 13, 2, 14, 1, 15)
SPREAD = (4, -4, 1, -1, 2, -2, 3, -3)
ARRIVAL = (1, -1, 4, -4, 2, -2, 3, -3, 5, -5, 6, -6, 7, -7, 8)


def step_kernel(
    acts_hbm, grads_hbm, master_hbm, first_hbm, second_hbm,
    master_out, first_out, second_out, wbuf,
    acts, slabs, cols, part, ysend, yrecv, zsend, zrecv,
    nsend, nrecv_p, nrecv_z,
    master, first, second,
    load_sem, own_sem, grad_sem, state_sem, swap_send, swap_recv,
    xsend_sem, xrecv_sem, ysend_sem, yrecv_sem, zsend_sem, zrecv_sem,
    nsend_sem, nrecv_sem, gsend_sem, gz_sem, gy_sem, known,
):
    z, y, x, c = (lax.axis_index(a) for a in DP_MP)
    dp = z * NY + y
    mp = x * NC + c

    def at_z(k):
        return (lax.rem(z + k, NZ), y, x, c)

    def at_y(k):
        return (z, lax.rem(y + k, NY), x, c)

    def in_plane(dy, dx, dc):
        return (z, lax.rem(y + dy, NY), lax.rem(x + dx, NX), lax.rem(c + dc, NC))

    def block_of(i, core):
        return lax.rem(z + jnp.where(core == 0, 8 + i, 7 - i), NZ)

    def send(src, dst, send_sem, recv_sem, device):
        copy = pltpu.make_async_remote_copy(
            src_ref=src, dst_ref=dst, send_sem=send_sem, recv_sem=recv_sem,
            device_id=device, device_id_type=MESH_ID,
        )
        copy.start()

    def wait_bytes(ref, sem):
        pltpu.make_async_copy(ref, ref, sem).wait()

    barrier = pltpu.get_barrier_semaphore()
    near = [in_plane(0, dx, dc) for dx in range(NX) for dc in range(NC) if (dx, dc) != (0, 0)]
    near += [at_y(k) for k in range(1, NY)]
    near += [(lax.rem(z + k, NZ), y, x, core) for k in (1, NZ - 1) for core in range(NC)]
    for device in near:
        pl.semaphore_signal(barrier, inc=1, device_id=device, device_id_type=MESH_ID)

    own_rows = pl.ds(pl.multiple_of(mp * 64, 64), 64)
    own_cols = pl.ds(pl.multiple_of(c * 256, 256), 256)
    for b in range(NZ):
        pltpu.make_async_copy(acts_hbm.at[:, pl.ds(b * 128, 128)], acts.at[b], load_sem).start()
    for which in range(2):
        lanes = pl.ds(pl.multiple_of(c * 256 + which * 128, 128), 128)
        pltpu.make_async_copy(grads_hbm.at[which], cols.at[:, lanes], grad_sem).start()
    for i in range(STEPS):
        lanes = pl.ds(pl.multiple_of(block_of(i, c) * 128, 128), 128)
        pltpu.make_async_copy(acts_hbm.at[:, lanes], slabs.at[i, own_rows], own_sem).start()
    pltpu.make_async_copy(master_hbm, master, state_sem.at[0]).start()
    pltpu.make_async_copy(first_hbm, first, state_sem.at[1]).start()
    pltpu.make_async_copy(second_hbm, second, state_sem.at[2]).start()

    wait_bytes(acts, load_sem)
    wait_bytes(cols.at[:, pl.ds(0, 256)], grad_sem)
    pl.semaphore_wait(barrier, len(near))

    def tell(level, devices):
        for device in devices:
            pl.semaphore_signal(known.at[level], inc=1, device_id=device, device_id_type=MESH_ID)

    tell(0, [at_y(k) for k in range(1, NY)] + [at_z(1), at_z(NZ - 1)])

    send(cols.at[:, own_cols], cols.at[:, own_cols], swap_send, swap_recv, in_plane(0, 0, 1))

    def gather_step(i):
        for core in range(NC):
            slab = acts.at[block_of(i, core)]
            for dx in range(1, NX):
                send(slab, slabs.at[i, own_rows], xsend_sem, xrecv_sem.at[i],
                     (z, y, lax.rem(x + dx, NX), core))
        slab = acts.at[block_of(i, 1 - c)]
        send(slab, slabs.at[i, own_rows], xsend_sem, xrecv_sem.at[i], (z, y, x, 1 - c))

    for i in range(AHEAD):
        gather_step(i)

    pl.semaphore_wait(known.at[0], NY + 1)
    tell(1, [at_z(2), at_z(NZ - 2)])
    wait_bytes(slabs.at[:, pl.ds(0, 64)], own_sem)
    wait_bytes(cols.at[:, pl.ds(0, 256)], swap_recv)

    def multiply(i):
        wait_bytes(slabs.at[i, pl.ds(0, 448)], xrecv_sem.at[i])

        @pl.when(i + AHEAD < STEPS)
        def _():
            gather_step(i + AHEAD)

        part[i % PARTS] = lax.dot_general(
            slabs[i], cols[...], (((0,), (0,)), ((), ())), preferred_element_type=jnp.float32
        )
        for k in range(1, NY):
            rows = pl.ds(pl.multiple_of(lax.rem(y + k, NY) * 32, 32), 32)
            piece = part[i % PARTS, rows, :].astype(jnp.bfloat16)
            for core in range(NC):
                for which in range(2):
                    at = core * 256 + which * 128
                    ysend[i, k - 1, core, which * 32 : which * 32 + 32, :] = piece[:, at : at + 128]
        for k in range(1, NY):
            send(ysend.at[i, k - 1], yrecv.at[i, k - 1], ysend_sem, yrecv_sem.at[i], at_y(k))

    def pass_on(i):
        wait_bytes(yrecv.at[i], yrecv_sem.at[i])
        rows = pl.ds(pl.multiple_of(y * 32, 32), 32)
        for core in range(NC):
            for which in range(2):
                at = core * 256 + which * 128
                total = part[i % PARTS, rows, at : at + 128]
                for k in range(NY - 1):
                    total += yrecv[i, k, core, which * 32 : which * 32 + 32, :].astype(jnp.float32)
                zsend[i, core, which * 32 : which * 32 + 32, :] = total.astype(jnp.bfloat16)
        k = jnp.where(c == 0, 8 + i, 7 - i)

        slot = 2 * i + c
        send(zsend.at[i, 0], zrecv.at[slot], zsend_sem, zrecv_sem.at[slot], (lax.rem(z + k, NZ), y, x, 0))

        @pl.when(k != 0)
        def _():
            send(zsend.at[i, 1], zrecv.at[slot], zsend_sem, zrecv_sem.at[slot], (lax.rem(z + k, NZ), y, x, 1))

    multiply(0)
    pl.semaphore_wait(known.at[1], 2)
    tell(2, [at_z(4), at_z(NZ - 4)])
    for i in range(1, LAG):
        multiply(i)
    pl.semaphore_wait(known.at[2], 2)

    def reduce_step(i, carry):
        multiply(i)
        pass_on(i - LAG)
        return carry

    lax.fori_loop(LAG, STEPS, reduce_step, 0)
    for i in range(STEPS - LAG, STEPS):
        pass_on(i)

    @pl.when(c == 1)
    def _():
        zrecv[NZ - 1] = zsend[STEPS - 1, 1]

    @pl.when(c == 0)
    def _():
        wait_bytes(zrecv.at[NZ - 1], zrecv_sem.at[NZ - 1])

    total = jnp.zeros((64, 128), jnp.float32)
    for slot in range(NZ - 1):
        wait_bytes(zrecv.at[slot], zrecv_sem.at[slot])
        total += zrecv[slot].astype(jnp.float32)
    total += zrecv[NZ - 1].astype(jnp.float32)

    tokens = 64 * NX * NC * NZ * NY
    gradient = total * (1.0 / tokens)

    squares = jnp.sum(gradient * gradient, axis=0, keepdims=True)
    nsend[0] = squares
    for dy in range(NY):
        for dx in range(NX):
            slot = nrecv_p.at[(dy * NX + dx) * NC + c]
            if (dy, dx) != (0, 0):
                send(nsend.at[0], slot, nsend_sem.at[0], nrecv_sem.at[0], (z, lax.rem(y + dy, NY), lax.rem(x + dx, NX), 1))

    @pl.when(c == 0)
    def _():
        send(nsend.at[0], nrecv_p.at[0], nsend_sem.at[0], nrecv_sem.at[0], (z, y, x, 1))

    @pl.when(c == 1)
    def _():
        nrecv_p[1] = squares
        wait_bytes(nrecv_p.at[pl.ds(0, PLANE - 1)], nrecv_sem.at[0])
        plane_sum = jnp.sum(nrecv_p[...], axis=0)
        nsend[1] = plane_sum
        nrecv_z[0] = plane_sum
        for k in Z_ORDER:
            for core in range(NC):
                send(nsend.at[1], nrecv_z.at[k], nsend_sem.at[1], nrecv_sem.at[1], (lax.rem(z + k, NZ), y, x, core))
        send(nsend.at[1], nrecv_z.at[0], nsend_sem.at[1], nrecv_sem.at[1], (z, y, x, 0))

    for n in range(3):
        wait_bytes((master, first, second)[n], state_sem.at[n])
    @pl.when(c == 0)
    def _():
        wait_bytes(nrecv_z, nrecv_sem.at[1])

    @pl.when(c == 1)
    def _():
        wait_bytes(nrecv_z.at[pl.ds(1, NZ - 1)], nrecv_sem.at[1])

    squares = jnp.sum(nrecv_z[...], axis=0)

    grad_norm = jnp.sqrt(jnp.sum(squares, axis=1, keepdims=True))
    limit = clip_scale * math.sqrt(2.0 * D * KV)
    clip_factor = jnp.minimum(jnp.float32(1.0), limit / (grad_norm + 1e-06))
    clipped_all = clip_factor * gradient
    for which in range(2):
        pick = pl.ds(which, 32, stride=2)
        clipped = clipped_all[which * 32 : which * 32 + 32]
        weights = master[pick, :]
        m = beta_first * first[pick, :] + (1.0 - beta_first) * clipped
        v = beta_second * second[pick, :] + (1.0 - beta_second) * clipped * clipped
        first_hat = m / (1.0 - beta_first**STEP)
        second_hat = v / (1.0 - beta_second**STEP)
        new = weights - learning_rate * (
            first_hat / (jnp.sqrt(second_hat) + adam_epsilon) + weight_decay * weights
        )
        master_out[pick, :] = new
        first_out[pick, :] = m
        second_out[pick, :] = v
    wbuf[dp] = master_out[...].astype(jnp.bfloat16)

    own = wbuf.at[dp]
    side = jnp.where(c == 0, 1, NZ - 1)

    def along(k):
        return lax.rem(z + side * (k + NZ), NZ)

    def pass_along(block, k, by):
        send(block, block, gsend_sem, gz_sem.at[ARRIVAL.index(k)], (along(by), y, x, c))

    def pass_across(block):
        for k in range(1, NY):
            send(block, block, gsend_sem, gy_sem, at_y(k))

    for k in SPREAD:
        pass_along(own, k, k)
    pass_across(own)
    for n, k in enumerate(ARRIVAL):
        got = wbuf.at[along(-k) * NY + y]
        wait_bytes(got, gz_sem.at[n])
        if k == 4:
            for by in (4, 3, 2, 1):
                pass_along(got, 4 + by, by)
        if k == -4:
            for by in (3, 2, 1):
                pass_along(got, -4 - by, -by)
        pass_across(got)
    wait_bytes(wbuf.at[pl.ds(0, 48)], gy_sem)

    wait_bytes(cols.at[:, pl.ds(0, 256)], swap_send)
    wait_bytes(slabs.at[pl.ds(0, 7)], xsend_sem)
    wait_bytes(yrecv, ysend_sem)
    wait_bytes(zrecv.at[pl.ds(0, NZ - 1)], zsend_sem)

    @pl.when(c == 0)
    def _():
        wait_bytes(zrecv.at[NZ - 1], zsend_sem)

    wait_bytes(nrecv_p.at[pl.ds(0, NY * NX - 1)], nsend_sem.at[0])

    @pl.when(c == 0)
    def _():
        wait_bytes(nrecv_p.at[0], nsend_sem.at[0])

    @pl.when(c == 1)
    def _():
        wait_bytes(nrecv_p.at[pl.ds(0, NC * NZ - 1)], nsend_sem.at[1])

    wait_bytes(wbuf.at[pl.ds(0, 63)], gsend_sem)


def write_kernel(*refs):
    ins, outs, sem = refs[:4], refs[4:8], refs[8]
    copies = [pltpu.make_async_copy(i, o, sem.at[n]) for n, (i, o) in enumerate(zip(ins, outs))]
    for copy in copies:
        copy.start()
    for copy in copies:
        copy.wait()


def on_device(activations, key_value_grads, master_weights, first_moment, second_moment):
    f32, bf16 = jnp.float32, jnp.bfloat16
    any_space = pl.BlockSpec(memory_space=pl.ANY)
    dma = pltpu.SemaphoreType.DMA
    vmem = pltpu.VMEM
    flat = [a.reshape(64, 128) for a in (master_weights, first_moment, second_moment)]
    in_vmem = pl.BlockSpec(memory_space=pltpu.VMEM)
    results = pl.pallas_call(
        step_kernel,
        out_shape=[vmem((64, 128), f32)] * 3 + [vmem((64, 64, 128), bf16)],
        in_specs=[any_space] * 5,
        out_specs=[in_vmem] * 4,
        scratch_shapes=[
            vmem((NZ, 64, 128), bf16),
            vmem((STEPS, 512, 128), bf16),
            vmem((512, 512), bf16),
            vmem((PARTS, 128, 512), f32),
            vmem((STEPS, NY - 1, NC, 64, 128), bf16),
            vmem((STEPS, NY - 1, NC, 64, 128), bf16),
            vmem((STEPS, NC, 64, 128), bf16),
            vmem((NZ, 64, 128), bf16),
            vmem((2, 1, 128), f32),
            vmem((PLANE, 1, 128), f32),
            vmem((NZ, 1, 128), f32),
            vmem((64, 128), f32),
            vmem((64, 128), f32),
            vmem((64, 128), f32),
            dma, dma, dma, dma((3,)), dma, dma,
            dma, dma((STEPS,)), dma, dma((STEPS,)), dma, dma((NZ,)),
            dma((2,)), dma((2,)), dma, dma((NZ - 1,)), dma,
            pltpu.SemaphoreType.REGULAR((3,)),
        ],
        compiler_params=pltpu.CompilerParams(collective_id=0, has_side_effects=True),
        name="adam_step",
    )(activations, key_value_grads, *flat)
    results = [pltpu.with_memory_space_constraint(r, pltpu.VMEM) for r in results]
    outs = pl.pallas_call(
        write_kernel,
        out_shape=[jax.ShapeDtypeStruct((64, 128), f32)] * 3 + [jax.ShapeDtypeStruct((64, 64, 128), bf16)],
        in_specs=[any_space] * 4,
        out_specs=[any_space] * 4,
        scratch_shapes=[dma((4,))],
        name="write_out",
    )(*results)
    return tuple(o.reshape(32, 2, 128) for o in outs[:3]) + (outs[3].reshape(D, 2, 128),)


def solution(mesh):
    split = Mesh(mesh.devices.reshape(NZ, NY, NX, NC), DP_MP)
    return jax.shard_map(
        on_device,
        mesh=split,
        in_specs=(
            P(DP_MP, None),
            P(None, DP, MP),
            P(DP, None, MP),
            P(DP, None, MP),
            P(DP, None, MP),
        ),
        out_specs=(P(DP, None, MP), P(DP, None, MP), P(DP, None, MP), P(None, None, MP)),
        check_vma=False,
    )
```

```python
import math

import jax
import jax.numpy as jnp
from jax import lax
from jax.experimental import pallas as pl
from jax.experimental.pallas import tpu as pltpu
from jax.sharding import Mesh
from jax.sharding import PartitionSpec as P

D = 2048
STEP = 8
KV = 1024
NZ, NY, NX, NC = 16, 4, 4, 2
STEPS = 8
AHEAD = 8
LAG = 2
PARTS = LAG + 1
DP = ("z", "y")
MP = ("x", "c")
DP_MP = ("z", "y", "x", "c")
MESH_ID = pl.DeviceIdType.MESH

beta_first = 0.9
beta_second = 0.95
adam_epsilon = 1e-08
learning_rate = 0.001
weight_decay = 0.1
clip_scale = 0.001

PLANE = [(dy, dx) for dy in (2, 1, 3, 0) for dx in (2, 1, 3, 0) if (dy, dx) != (0, 0)]
Z_ORDER = (8, 7, 9, 6, 10, 5, 11, 4, 12, 3, 13, 2, 14, 1, 15)
ONWARD = {0: (4, -4, 1, -1, 2, -2, 3, -3), 4: (8, 7, 6, 5), -4: (-7, -6, -5)}
ARRIVAL = (1, -1, 4, -4, 2, -2, 3, -3, 5, -5, 6, -6, 7, -7, 8)
ACROSS = (2, 1, 3)
YSENDS = (2, 1, 3)
XSENDS = (2, 1, 3)


def step_kernel(
    acts_hbm, grads_hbm, master_hbm, first_hbm, second_hbm,
    master_out, first_out, second_out, wbuf,
    acts, slabs, cols, part, ysend, yrecv, zsend, zrecv,
    nsend, nrecv_p, nrecv_z, nsum,
    state, gsum, half,
    load_sem, own_sem, grad_sem, state_sem, swap_send, swap_recv,
    xsend_sem, xrecv_sem, ysend_sem, yrecv_sem, zsend_sem, zrecv_sem, half_send, half_recv,
    nsend_sem, nrecv_sem, gsend_sem, gz_sem, gy_sem, known,
):
    z, y, x, c = (lax.axis_index(a) for a in DP_MP)
    dp = z * NY + y
    mp = x * NC + c

    def at_z(k):
        return (lax.rem(z + k, NZ), y, x, c)

    def at_y(k):
        return (z, lax.rem(y + k, NY), x, c)

    def in_plane(dy, dx, dc):
        return (z, lax.rem(y + dy, NY), lax.rem(x + dx, NX), lax.rem(c + dc, NC))

    def block_of(i, core):
        return lax.rem(z + jnp.where(core == 0, 8 + i, 7 - i), NZ)

    def send(src, dst, send_sem, recv_sem, device):
        copy = pltpu.make_async_remote_copy(
            src_ref=src, dst_ref=dst, send_sem=send_sem, recv_sem=recv_sem,
            device_id=device, device_id_type=MESH_ID,
        )
        copy.start()

    def wait_bytes(ref, sem):
        pltpu.make_async_copy(ref, ref, sem).wait()

    barrier = pltpu.get_barrier_semaphore()
    near = [in_plane(0, dx, dc) for dx in range(NX) for dc in range(NC) if (dx, dc) != (0, 0)]
    near += [at_y(k) for k in range(1, NY)]
    near += [(lax.rem(z + k, NZ), y, x, core) for k in (1, NZ - 1) for core in range(NC)]
    for device in near:
        pl.semaphore_signal(barrier, inc=1, device_id=device, device_id_type=MESH_ID)

    own_rows = pl.ds(pl.multiple_of(mp * 64, 64), 64)
    own_cols = pl.ds(pl.multiple_of(c * 256, 256), 256)
    for b in range(NZ):
        pltpu.make_async_copy(acts_hbm.at[:, pl.ds(b * 128, 128)], acts.at[b], load_sem).start()
    for which in range(2):
        lanes = pl.ds(pl.multiple_of(c * 256 + which * 128, 128), 128)
        pltpu.make_async_copy(grads_hbm.at[which], cols.at[:, lanes], grad_sem).start()
    for i in range(STEPS):
        lanes = pl.ds(pl.multiple_of(block_of(i, c) * 128, 128), 128)
        pltpu.make_async_copy(acts_hbm.at[:, lanes], slabs.at[i, own_rows], own_sem).start()
    for n, ref in enumerate((master_hbm, first_hbm, second_hbm)):
        pltpu.make_async_copy(ref, state.at[n], state_sem).start()

    wait_bytes(acts, load_sem)
    wait_bytes(cols.at[:, pl.ds(0, 256)], grad_sem)
    pl.semaphore_wait(barrier, len(near))

    def tell(level, devices):
        for device in devices:
            pl.semaphore_signal(known.at[level], inc=1, device_id=device, device_id_type=MESH_ID)

    tell(0, [at_y(k) for k in range(1, NY)] + [at_z(1), at_z(NZ - 1)])

    send(cols.at[:, own_cols], cols.at[:, own_cols], swap_send, swap_recv, in_plane(0, 0, 1))

    def gather_step(i):
        for core in range(NC):
            slab = acts.at[block_of(i, core)]
            for dx in XSENDS:
                send(slab, slabs.at[i, own_rows], xsend_sem, xrecv_sem.at[i],
                     (z, y, lax.rem(x + dx, NX), core))
        slab = acts.at[block_of(i, 1 - c)]
        send(slab, slabs.at[i, own_rows], xsend_sem, xrecv_sem.at[i], (z, y, x, 1 - c))

    for i in range(AHEAD):
        gather_step(i)

    pl.semaphore_wait(known.at[0], NY + 1)
    tell(1, [at_z(2), at_z(NZ - 2)])
    wait_bytes(slabs.at[:, pl.ds(0, 64)], own_sem)
    wait_bytes(state, state_sem)
    wait_bytes(cols.at[:, pl.ds(0, 256)], swap_recv)

    def multiply(i):
        wait_bytes(slabs.at[i, pl.ds(0, 448)], xrecv_sem.at[i])

        @pl.when(i + AHEAD < STEPS)
        def _():
            gather_step(i + AHEAD)

        part[i % PARTS] = lax.dot_general(
            slabs[i], cols[...], (((0,), (0,)), ((), ())), preferred_element_type=jnp.float32
        )
        for k in range(1, NY):
            rows = pl.ds(pl.multiple_of(lax.rem(y + k, NY) * 32, 32), 32)
            piece = part[i % PARTS, rows, :].astype(jnp.bfloat16)
            for core in range(NC):
                for which in range(2):
                    at = core * 256 + which * 128
                    ysend[i, k - 1, core, which * 32 : which * 32 + 32, :] = piece[:, at : at + 128]
        for k in YSENDS:
            send(ysend.at[i, k - 1], yrecv.at[i, k - 1], ysend_sem, yrecv_sem.at[i], at_y(k))

    def pass_on(i):
        wait_bytes(yrecv.at[i], yrecv_sem.at[i])
        rows = pl.ds(pl.multiple_of(y * 32, 32), 32)
        for core in range(NC):
            for which in range(2):
                at = core * 256 + which * 128
                total = part[i % PARTS, rows, at : at + 128]
                for k in range(NY - 1):
                    total += yrecv[i, k, core, which * 32 : which * 32 + 32, :].astype(jnp.float32)
                zsend[i, core, which * 32 : which * 32 + 32, :] = total.astype(jnp.bfloat16)
        k = jnp.where(c == 0, 8 + i, 7 - i)

        slot = 2 * i + c

        @pl.when(k != 0)
        def _():
            send(zsend.at[i], zrecv.at[slot], zsend_sem, zrecv_sem.at[slot], (lax.rem(z + k, NZ), y, x, 1))

    pl.semaphore_wait(known.at[1], 2)
    tell(2, [at_z(4), at_z(NZ - 4)])
    for i in range(LAG):
        multiply(i)
    pl.semaphore_wait(known.at[2], 2)

    def reduce_step(i, carry):
        multiply(i)
        pass_on(i - LAG)
        return carry

    lax.fori_loop(LAG, STEPS, reduce_step, 0)
    for i in range(STEPS - LAG, STEPS):
        pass_on(i)

    def clip(sums):
        grad_norm = jnp.sqrt(jnp.sum(sums, axis=1, keepdims=True))
        limit = clip_scale * math.sqrt(2.0 * D * KV)
        return jnp.minimum(jnp.float32(1.0), limit / (grad_norm + 1e-06))

    def adam(gradient, clip_factor, held, new_out, first_to, second_to):
        clipped_all = clip_factor * gradient
        for which in range(2):
            pick = pl.ds(which, 32, stride=2)
            clipped = clipped_all[which * 32 : which * 32 + 32]
            weights = held[0, pick, :]
            m = beta_first * held[1, pick, :] + (1.0 - beta_first) * clipped
            v = beta_second * held[2, pick, :] + (1.0 - beta_second) * clipped * clipped
            first_hat = m / (1.0 - beta_first**STEP)
            second_hat = v / (1.0 - beta_second**STEP)
            new_out[pick, :] = weights - learning_rate * (
                first_hat / (jnp.sqrt(second_hat) + adam_epsilon) + weight_decay * weights
            )
            if first_to is not None:
                first_to[pick, :] = m
                second_to[pick, :] = v

    scale = 1.0 / (64 * NX * NC * NZ * NY)

    @pl.when(c == 0)
    def _():
        wait_bytes(gsum, half_recv)
        wait_bytes(nrecv_z, nrecv_sem.at[1])
        factor = clip(jnp.sum(nrecv_z[...], axis=0))
        adam(gsum[...], factor, state, master_out, first_out, second_out)
        wait_bytes(zrecv.at[pl.ds(0, STEPS)], zsend_sem)

    @pl.when(c == 1)
    def _():
        totals = [zsend[STEPS - 1, core].astype(jnp.float32) for core in range(NC)]
        for slot in range(NZ - 1):
            wait_bytes(zrecv.at[slot], zrecv_sem.at[slot])
            for core in range(NC):
                totals[core] += zrecv[slot, core].astype(jnp.float32)
        gradients = [total * scale for total in totals]
        squares = jnp.sum(gradients[0] * gradients[0] + gradients[1] * gradients[1], axis=0, keepdims=True)
        nsend[0] = squares
        nrecv_p[0] = squares
        for dy, dx in PLANE:
            send(nsend.at[0], nrecv_p.at[dy * NX + dx], nsend_sem.at[0], nrecv_sem.at[0],
                 (z, lax.rem(y + dy, NY), lax.rem(x + dx, NX), 1))
        half[...] = gradients[0]
        gsum[...] = gradients[1]
        send(half, gsum, half_send, half_recv, (z, y, x, 0))
        wait_bytes(nrecv_p.at[pl.ds(1, NY * NX - 1)], nrecv_sem.at[0])
        plane_sum = jnp.sum(nrecv_p[...], axis=0)
        nsend[1] = plane_sum
        nrecv_z[0] = plane_sum
        for core in (1, 0):
            for k in Z_ORDER:
                send(nsend.at[1], nrecv_z.at[k], nsend_sem.at[1], nrecv_sem.at[1], (lax.rem(z + k, NZ), y, x, core))
        send(nsend.at[1], nrecv_z.at[0], nsend_sem.at[1], nrecv_sem.at[1], (z, y, x, 0))
        wait_bytes(nrecv_z.at[pl.ds(1, NZ - 1)], nrecv_sem.at[1])
        factor = clip(jnp.sum(nrecv_z[...], axis=0))
        adam(gsum[...], factor, state, master_out, first_out, second_out)
        wait_bytes(zrecv.at[pl.ds(0, STEPS - 1)], zsend_sem)
        wait_bytes(half, half_send)
        wait_bytes(nrecv_p.at[pl.ds(1, NY * NX - 1)], nsend_sem.at[0])
        wait_bytes(nsum.at[pl.ds(0, NC * NZ - 1)], nsend_sem.at[1])

    wbuf[dp] = master_out[...].astype(jnp.bfloat16)
    side = jnp.where(c == 0, 1, NZ - 1)

    def along(k):
        return lax.rem(z + side * (k + NZ), NZ)

    def pass_along(block, k, by):
        send(block, block, gsend_sem, gz_sem.at[ARRIVAL.index(k)], (along(by), y, x, c))

    def pass_across(block):
        for k in ACROSS:
            send(block, block, gsend_sem, gy_sem, at_y(k))

    own = wbuf.at[dp]
    for k in ONWARD[0]:
        pass_along(own, k, k)
    pass_across(own)
    for n, k in enumerate(ARRIVAL):
        got = wbuf.at[along(-k) * NY + y]
        wait_bytes(got, gz_sem.at[n])
        for further in ONWARD.get(k, ()):
            pass_along(got, further, further - k)
        pass_across(got)
    wait_bytes(wbuf.at[pl.ds(0, 48)], gy_sem)
    wait_bytes(wbuf.at[pl.ds(0, 63)], gsend_sem)
    wait_bytes(cols.at[:, pl.ds(0, 256)], swap_send)
    wait_bytes(slabs.at[pl.ds(0, 7)], xsend_sem)
    wait_bytes(yrecv, ysend_sem)


def write_kernel(*refs):
    ins, outs, sem = refs[:4], refs[4:8], refs[8]
    copies = [pltpu.make_async_copy(i, o, sem.at[n]) for n, (i, o) in enumerate(zip(ins, outs))]
    for copy in copies:
        copy.start()
    for copy in copies:
        copy.wait()


def on_device(activations, key_value_grads, master_weights, first_moment, second_moment):
    f32, bf16 = jnp.float32, jnp.bfloat16
    any_space = pl.BlockSpec(memory_space=pl.ANY)
    dma = pltpu.SemaphoreType.DMA
    vmem = pltpu.VMEM
    flat = [a.reshape(64, 128) for a in (master_weights, first_moment, second_moment)]
    in_vmem = pl.BlockSpec(memory_space=pltpu.VMEM)
    results = pl.pallas_call(
        step_kernel,
        out_shape=[vmem((64, 128), f32)] * 3 + [vmem((64, 64, 128), bf16)],
        in_specs=[any_space] * 5,
        out_specs=[in_vmem] * 4,
        scratch_shapes=[
            vmem((NZ, 64, 128), bf16),
            vmem((STEPS, 512, 128), bf16),
            vmem((512, 512), bf16),
            vmem((PARTS, 128, 512), f32),
            vmem((STEPS, NY - 1, NC, 64, 128), bf16),
            vmem((STEPS, NY - 1, NC, 64, 128), bf16),
            vmem((STEPS, NC, 64, 128), bf16),
            vmem((NZ, NC, 64, 128), bf16),
            vmem((2, 1, 128), f32),
            vmem((NY * NX, 1, 128), f32),
            vmem((NZ, 1, 128), f32),
            vmem((NZ * NC, 1, 128), f32),
            vmem((3, 64, 128), f32),
            vmem((64, 128), f32),
            vmem((64, 128), f32),
            dma, dma, dma, dma, dma, dma,
            dma, dma((STEPS,)), dma, dma((STEPS,)), dma, dma((NZ,)), dma, dma,
            dma((2,)), dma((2,)), dma, dma((NZ - 1,)), dma,
            pltpu.SemaphoreType.REGULAR((3,)),
        ],
        compiler_params=pltpu.CompilerParams(collective_id=0, has_side_effects=True),
        name="adam_step",
    )(activations, key_value_grads, *flat)
    results = [pltpu.with_memory_space_constraint(r, pltpu.VMEM) for r in results]
    outs = pl.pallas_call(
        write_kernel,
        out_shape=[jax.ShapeDtypeStruct((64, 128), f32)] * 3 + [jax.ShapeDtypeStruct((64, 64, 128), bf16)],
        in_specs=[any_space] * 4,
        out_specs=[any_space] * 4,
        scratch_shapes=[dma((4,))],
        name="write_out",
    )(*results)
    return tuple(o.reshape(32, 2, 128) for o in outs[:3]) + (outs[3].reshape(D, 2, 128),)


def solution(mesh):
    split = Mesh(mesh.devices.reshape(NZ, NY, NX, NC), DP_MP)
    return jax.shard_map(
        on_device,
        mesh=split,
        in_specs=(
            P(DP_MP, None),
            P(None, DP, MP),
            P(DP, None, MP),
            P(DP, None, MP),
            P(DP, None, MP),
        ),
        out_specs=(P(DP, None, MP), P(DP, None, MP), P(DP, None, MP), P(None, None, MP)),
        check_vma=False,
    )
```

```python
import math

import jax
import jax.numpy as jnp
from jax import lax
from jax.experimental import pallas as pl
from jax.experimental.pallas import tpu as pltpu
from jax.sharding import Mesh
from jax.sharding import PartitionSpec as P

D = 2048
STEP = 8
KV = 1024
NZ, NY, NX, NC = 16, 4, 4, 2
STEPS = 8
AHEAD = 8
LAG = 2
SWAP_AT = 2
PARTS = LAG + 1
DP = ("z", "y")
MP = ("x", "c")
DP_MP = ("z", "y", "x", "c")
MESH_ID = pl.DeviceIdType.MESH

beta_first = 0.9
beta_second = 0.95
adam_epsilon = 1e-08
learning_rate = 0.001
weight_decay = 0.1
clip_scale = 0.001

PLANE = [(dy, dx) for dy in (2, 1, 3, 0) for dx in (2, 1, 3, 0) if (dy, dx) != (0, 0)]
Z_ORDER = (8, 7, 9, 6, 10, 5, 11, 4, 12, 3, 13, 2, 14, 1, 15)
ONWARD = {0: (4, -4, 1, -1, 2, -2, 3, -3), 4: (8, 7, 6, 5), -4: (-7, -6, -5)}
ARRIVAL = (1, -1, 4, -4, 2, -2, 3, -3, 5, -5, 6, -6, 7, -7, 8)
ACROSS = (2, 1, 3)
YSENDS = (2, 1, 3)
XSENDS = (2, 1, 3)


def step_kernel(
    acts_hbm, grads_hbm, master_hbm, first_hbm, second_hbm,
    master_out, first_out, second_out, wbuf,
    acts, slabs, cols, part, ysend, yrecv, zsend, zrecv,
    nsend, nrecv_p, nrecv_z, nsum,
    state, gsum, half,
    load_sem, own_sem, grad_sem, state_sem, swap_send, swap_recv,
    xsend_sem, xrecv_sem, ysend_sem, yrecv_sem, zsend_sem, zrecv_sem, half_send, half_recv,
    nsend_sem, nrecv_sem, gsend_sem, gz_sem, gy_sem, known,
):
    z, y, x, c = (lax.axis_index(a) for a in DP_MP)
    dp = z * NY + y
    mp = x * NC + c

    def at_z(k):
        return (lax.rem(z + k, NZ), y, x, c)

    def at_y(k):
        return (z, lax.rem(y + k, NY), x, c)

    def in_plane(dy, dx, dc):
        return (z, lax.rem(y + dy, NY), lax.rem(x + dx, NX), lax.rem(c + dc, NC))

    def block_of(i, core):
        return lax.rem(z + jnp.where(core == 0, 8 + i, 7 - i), NZ)

    def send(src, dst, send_sem, recv_sem, device):
        copy = pltpu.make_async_remote_copy(
            src_ref=src, dst_ref=dst, send_sem=send_sem, recv_sem=recv_sem,
            device_id=device, device_id_type=MESH_ID,
        )
        copy.start()

    def wait_bytes(ref, sem):
        pltpu.make_async_copy(ref, ref, sem).wait()

    barrier = pltpu.get_barrier_semaphore()
    near = [in_plane(0, dx, dc) for dx in range(NX) for dc in range(NC) if (dx, dc) != (0, 0)]
    near += [at_y(k) for k in range(1, NY)]
    near += [(lax.rem(z + k, NZ), y, x, core) for k in (1, NZ - 1) for core in range(NC)]
    for device in near:
        pl.semaphore_signal(barrier, inc=1, device_id=device, device_id_type=MESH_ID)

    own_rows = pl.ds(pl.multiple_of(mp * 64, 64), 64)
    own_cols = pl.ds(pl.multiple_of(c * 256, 256), 256)
    for b in range(NZ):
        pltpu.make_async_copy(acts_hbm.at[:, pl.ds(b * 128, 128)], acts.at[b], load_sem).start()
    for which in range(2):
        lanes = pl.ds(pl.multiple_of(c * 256 + which * 128, 128), 128)
        pltpu.make_async_copy(grads_hbm.at[which], cols.at[:, lanes], grad_sem).start()
    for i in range(STEPS):
        lanes = pl.ds(pl.multiple_of(block_of(i, c) * 128, 128), 128)
        pltpu.make_async_copy(acts_hbm.at[:, lanes], slabs.at[i, own_rows], own_sem).start()
    for n, ref in enumerate((master_hbm, first_hbm, second_hbm)):
        pltpu.make_async_copy(ref, state.at[n], state_sem).start()

    wait_bytes(acts, load_sem)
    pl.semaphore_wait(barrier, len(near))

    def tell(level, devices):
        for device in devices:
            pl.semaphore_signal(known.at[level], inc=1, device_id=device, device_id_type=MESH_ID)

    tell(0, [at_y(k) for k in range(1, NY)] + [at_z(1), at_z(NZ - 1)])


    def gather_step(i):
        for core in range(NC):
            slab = acts.at[block_of(i, core)]
            for dx in XSENDS:
                send(slab, slabs.at[i, own_rows], xsend_sem, xrecv_sem.at[i],
                     (z, y, lax.rem(x + dx, NX), core))
        slab = acts.at[block_of(i, 1 - c)]
        send(slab, slabs.at[i, own_rows], xsend_sem, xrecv_sem.at[i], (z, y, x, 1 - c))

    for i in range(AHEAD):
        if i == SWAP_AT:
            wait_bytes(cols.at[:, pl.ds(0, 256)], grad_sem)
            send(cols.at[:, own_cols], cols.at[:, own_cols], swap_send, swap_recv, in_plane(0, 0, 1))
        gather_step(i)

    pl.semaphore_wait(known.at[0], NY + 1)
    tell(1, [at_z(2), at_z(NZ - 2)])
    wait_bytes(slabs.at[:, pl.ds(0, 64)], own_sem)
    wait_bytes(state, state_sem)
    wait_bytes(cols.at[:, pl.ds(0, 256)], swap_recv)

    def multiply(i):
        wait_bytes(slabs.at[i, pl.ds(0, 448)], xrecv_sem.at[i])

        @pl.when(i + AHEAD < STEPS)
        def _():
            gather_step(i + AHEAD)

        part[i % PARTS] = lax.dot_general(
            slabs[i], cols[...], (((0,), (0,)), ((), ())), preferred_element_type=jnp.float32
        )
        for k in range(1, NY):
            rows = pl.ds(pl.multiple_of(lax.rem(y + k, NY) * 32, 32), 32)
            piece = part[i % PARTS, rows, :].astype(jnp.bfloat16)
            for core in range(NC):
                for which in range(2):
                    at = core * 256 + which * 128
                    ysend[i, k - 1, core, which * 32 : which * 32 + 32, :] = piece[:, at : at + 128]
        for k in YSENDS:
            send(ysend.at[i, k - 1], yrecv.at[i, k - 1], ysend_sem, yrecv_sem.at[i], at_y(k))

    def pass_on(i):
        wait_bytes(yrecv.at[i], yrecv_sem.at[i])
        rows = pl.ds(pl.multiple_of(y * 32, 32), 32)
        for core in range(NC):
            for which in range(2):
                at = core * 256 + which * 128
                total = part[i % PARTS, rows, at : at + 128]
                for k in range(NY - 1):
                    total += yrecv[i, k, core, which * 32 : which * 32 + 32, :].astype(jnp.float32)
                zsend[i, core, which * 32 : which * 32 + 32, :] = total.astype(jnp.bfloat16)
        k = jnp.where(c == 0, 8 + i, 7 - i)

        slot = 2 * i + c

        @pl.when(k != 0)
        def _():
            send(zsend.at[i], zrecv.at[slot], zsend_sem, zrecv_sem.at[slot], (lax.rem(z + k, NZ), y, x, 1))

    pl.semaphore_wait(known.at[1], 2)
    tell(2, [at_z(4), at_z(NZ - 4)])
    for i in range(LAG):
        multiply(i)
    pl.semaphore_wait(known.at[2], 2)

    def reduce_step(i, carry):
        multiply(i)
        pass_on(i - LAG)
        return carry

    lax.fori_loop(LAG, STEPS, reduce_step, 0)
    for i in range(STEPS - LAG, STEPS):
        pass_on(i)

    def clip(sums):
        grad_norm = jnp.sqrt(jnp.sum(sums, axis=1, keepdims=True))
        limit = clip_scale * math.sqrt(2.0 * D * KV)
        return jnp.minimum(jnp.float32(1.0), limit / (grad_norm + 1e-06))

    def adam(gradient, clip_factor, held, new_out, first_to, second_to):
        clipped_all = clip_factor * gradient
        for which in range(2):
            pick = pl.ds(which, 32, stride=2)
            clipped = clipped_all[which * 32 : which * 32 + 32]
            weights = held[0, pick, :]
            m = beta_first * held[1, pick, :] + (1.0 - beta_first) * clipped
            v = beta_second * held[2, pick, :] + (1.0 - beta_second) * clipped * clipped
            first_hat = m / (1.0 - beta_first**STEP)
            second_hat = v / (1.0 - beta_second**STEP)
            new_out[pick, :] = weights - learning_rate * (
                first_hat / (jnp.sqrt(second_hat) + adam_epsilon) + weight_decay * weights
            )
            if first_to is not None:
                first_to[pick, :] = m
                second_to[pick, :] = v

    scale = 1.0 / (64 * NX * NC * NZ * NY)

    @pl.when(c == 0)
    def _():
        wait_bytes(gsum, half_recv)
        wait_bytes(nrecv_z, nrecv_sem.at[1])
        factor = clip(jnp.sum(nrecv_z[...], axis=0))
        adam(gsum[...], factor, state, master_out, first_out, second_out)
        wait_bytes(zrecv.at[pl.ds(0, STEPS)], zsend_sem)

    @pl.when(c == 1)
    def _():
        totals = [zsend[STEPS - 1, core].astype(jnp.float32) for core in range(NC)]
        for slot in range(NZ - 1):
            wait_bytes(zrecv.at[slot], zrecv_sem.at[slot])
            for core in range(NC):
                totals[core] += zrecv[slot, core].astype(jnp.float32)
        gradients = [total * scale for total in totals]
        squares = jnp.sum(gradients[0] * gradients[0] + gradients[1] * gradients[1], axis=0, keepdims=True)
        nsend[0] = squares
        nrecv_p[0] = squares
        for dy, dx in PLANE:
            send(nsend.at[0], nrecv_p.at[dy * NX + dx], nsend_sem.at[0], nrecv_sem.at[0],
                 (z, lax.rem(y + dy, NY), lax.rem(x + dx, NX), 1))
        half[...] = gradients[0]
        gsum[...] = gradients[1]
        send(half, gsum, half_send, half_recv, (z, y, x, 0))
        wait_bytes(nrecv_p.at[pl.ds(1, NY * NX - 1)], nrecv_sem.at[0])
        plane_sum = jnp.sum(nrecv_p[...], axis=0)
        nsend[1] = plane_sum
        nrecv_z[0] = plane_sum
        for k in Z_ORDER:
            for core in (0, 1):
                send(nsend.at[1], nrecv_z.at[k], nsend_sem.at[1], nrecv_sem.at[1], (lax.rem(z + k, NZ), y, x, core))
        send(nsend.at[1], nrecv_z.at[0], nsend_sem.at[1], nrecv_sem.at[1], (z, y, x, 0))
        wait_bytes(nrecv_z.at[pl.ds(1, NZ - 1)], nrecv_sem.at[1])
        factor = clip(jnp.sum(nrecv_z[...], axis=0))
        adam(gsum[...], factor, state, master_out, first_out, second_out)
        wait_bytes(zrecv.at[pl.ds(0, STEPS - 1)], zsend_sem)
        wait_bytes(half, half_send)
        wait_bytes(nrecv_p.at[pl.ds(1, NY * NX - 1)], nsend_sem.at[0])
        wait_bytes(nsum.at[pl.ds(0, NC * NZ - 1)], nsend_sem.at[1])

    wbuf[dp] = master_out[...].astype(jnp.bfloat16)
    side = jnp.where(c == 0, 1, NZ - 1)

    def along(k):
        return lax.rem(z + side * (k + NZ), NZ)

    def pass_along(block, k, by):
        send(block, block, gsend_sem, gz_sem.at[ARRIVAL.index(k)], (along(by), y, x, c))

    def pass_across(block):
        for k in ACROSS:
            send(block, block, gsend_sem, gy_sem, at_y(k))

    own = wbuf.at[dp]
    for k in ONWARD[0]:
        pass_along(own, k, k)
    pass_across(own)
    for n, k in enumerate(ARRIVAL):
        got = wbuf.at[along(-k) * NY + y]
        wait_bytes(got, gz_sem.at[n])
        for further in ONWARD.get(k, ()):
            pass_along(got, further, further - k)
        pass_across(got)
    wait_bytes(wbuf.at[pl.ds(0, 48)], gy_sem)
    wait_bytes(wbuf.at[pl.ds(0, 63)], gsend_sem)
    wait_bytes(cols.at[:, pl.ds(0, 256)], swap_send)
    wait_bytes(slabs.at[pl.ds(0, 7)], xsend_sem)
    wait_bytes(yrecv, ysend_sem)


def write_kernel(*refs):
    ins, outs, sem = refs[:4], refs[4:8], refs[8]
    copies = [pltpu.make_async_copy(i, o, sem.at[n]) for n, (i, o) in enumerate(zip(ins, outs))]
    for copy in copies:
        copy.start()
    for copy in copies:
        copy.wait()


def on_device(activations, key_value_grads, master_weights, first_moment, second_moment):
    f32, bf16 = jnp.float32, jnp.bfloat16
    any_space = pl.BlockSpec(memory_space=pl.ANY)
    dma = pltpu.SemaphoreType.DMA
    vmem = pltpu.VMEM
    flat = [a.reshape(64, 128) for a in (master_weights, first_moment, second_moment)]
    in_vmem = pl.BlockSpec(memory_space=pltpu.VMEM)
    results = pl.pallas_call(
        step_kernel,
        out_shape=[vmem((64, 128), f32)] * 3 + [vmem((64, 64, 128), bf16)],
        in_specs=[any_space] * 5,
        out_specs=[in_vmem] * 4,
        scratch_shapes=[
            vmem((NZ, 64, 128), bf16),
            vmem((STEPS, 512, 128), bf16),
            vmem((512, 512), bf16),
            vmem((PARTS, 128, 512), f32),
            vmem((STEPS, NY - 1, NC, 64, 128), bf16),
            vmem((STEPS, NY - 1, NC, 64, 128), bf16),
            vmem((STEPS, NC, 64, 128), bf16),
            vmem((NZ, NC, 64, 128), bf16),
            vmem((2, 1, 128), f32),
            vmem((NY * NX, 1, 128), f32),
            vmem((NZ, 1, 128), f32),
            vmem((NZ * NC, 1, 128), f32),
            vmem((3, 64, 128), f32),
            vmem((64, 128), f32),
            vmem((64, 128), f32),
            dma, dma, dma, dma, dma, dma,
            dma, dma((STEPS,)), dma, dma((STEPS,)), dma, dma((NZ,)), dma, dma,
            dma((2,)), dma((2,)), dma, dma((NZ - 1,)), dma,
            pltpu.SemaphoreType.REGULAR((3,)),
        ],
        compiler_params=pltpu.CompilerParams(collective_id=0, has_side_effects=True),
        name="adam_step",
    )(activations, key_value_grads, *flat)
    results = [pltpu.with_memory_space_constraint(r, pltpu.VMEM) for r in results]
    outs = pl.pallas_call(
        write_kernel,
        out_shape=[jax.ShapeDtypeStruct((64, 128), f32)] * 3 + [jax.ShapeDtypeStruct((64, 64, 128), bf16)],
        in_specs=[any_space] * 4,
        out_specs=[any_space] * 4,
        scratch_shapes=[dma((4,))],
        name="write_out",
    )(*results)
    return tuple(o.reshape(32, 2, 128) for o in outs[:3]) + (outs[3].reshape(D, 2, 128),)


def solution(mesh):
    split = Mesh(mesh.devices.reshape(NZ, NY, NX, NC), DP_MP)
    return jax.shard_map(
        on_device,
        mesh=split,
        in_specs=(
            P(DP_MP, None),
            P(None, DP, MP),
            P(DP, None, MP),
            P(DP, None, MP),
            P(DP, None, MP),
        ),
        out_specs=(P(DP, None, MP), P(DP, None, MP), P(DP, None, MP), P(None, None, MP)),
        check_vma=False,
    )
```
